32 devices in a mesh: ga: 2 (over core), band: 16 (over z, y, x).
Axes of the slice: x: 2, y: 2, z: 4, core: 2. Of those that a mesh axis runs over, the one named last changes fastest.
Arguments:
- orbitals: bfloat16 [1024, 2, 16384], P('band', None, 'ga'), may hold values from -6 to 6
- projectors: bfloat16 [864, 2, 16384], P(None, None, ('ga', 'band')), may hold values from -0.03125 to 0.03125
- coupling: float32 [4, 18, 18], replicated, may hold values from -6 to 6
- species: int32 [48], replicated, may hold values from 0 to 3
- offsets: int32 [48], replicated, may hold values from 0 to 846, as said below
Outputs:
- applied: bfloat16 [1024, 2, 16384], P('band', None, 'ga')
The draws below stay inside these ranges and needn't reach their ends.
Inputs may be any that keep to these rules, and one draw needn't show every extreme that they name: Each atom's 18 projectors are the 18 consecutive rows of projectors starting at its offset; offsets are multiples of 18, and the atoms' blocks are distinct and cover all 864 rows.
All inputs are finite; a program needn't handle non-finite values.
Results may differ from the reference program's by a relative error of at most 0.0049.
Values may be sent and summed in bfloat16 or wider, within the bound.
A program may use at most 64 MiB of HBM per device.

```python
import jax
import jax.numpy as jnp
from jax import lax

NBANDS = 1024
PROJ = 18
NSP = 4
ATOMS = 48
NPW = 16384
NKB = 864


def draw_offsets(key, part):
    order = jax.random.permutation(key, ATOMS)
    return (order * PROJ).astype(jnp.int32)


def plant(drawn, stream_key, smallest, largest):
    extent = drawn.shape
    spot = [jax.random.randint(jax.random.fold_in(stream_key, axis), (), 0, extent[axis]) for axis in range(len(extent))]
    drawn = drawn.at[tuple(spot)].set(smallest)
    longest = extent.index(max(extent))
    spot[longest] = (spot[longest] + 1) % extent[longest]
    return drawn.at[tuple(spot)].set(largest)


def block_scale(key, dims, cuts, least, top_value):
    gain = 1.0
    for axis_at, blocks in cuts:
        heights = jax.random.uniform(jax.random.fold_in(jax.random.fold_in(key, 6), axis_at), (blocks,), jnp.float32, least / len(cuts), top_value / len(cuts))
        gain = gain * jnp.repeat(jnp.exp(heights), dims[axis_at] // blocks).reshape((-1,) + (1,) * (len(dims) - 1 - axis_at))
    return gain


def normal_values(stream_key, shape, spread, most, pieces=(), held_as=jnp.bfloat16):
    values = spread * jax.random.normal(stream_key, shape, jnp.float32)
    if pieces:
        values = values * block_scale(stream_key, shape, pieces, -0.22, 0.18)
    return jnp.clip(values, -most, most).astype(held_as)


def setup_inputs(seed: int = 0) -> dict:
    arg_keys = jax.random.split(jax.random.key(seed), 6)
    return {
        "orbitals": normal_values(arg_keys[0], (NBANDS, 2, NPW), 1.0, 6.0, ((0, 16), (2, 2))),
        "projectors": normal_values(arg_keys[1], (NKB, 2, NPW), (2 * NPW) ** -0.5, 0.03125, ((2, 32),)),
        "coupling": normal_values(arg_keys[2], (NSP, PROJ, PROJ), ((NPW / (18 * NKB)) ** 0.5), 6.0, (), jnp.float32),
        "species": plant(jax.random.randint(arg_keys[3], (ATOMS,), 0, NSP), jax.random.fold_in(arg_keys[3], 1), 0, NSP - 1).astype(jnp.int32),
        "offsets": draw_offsets(jax.random.fold_in(arg_keys[5], 71), 0),
    }


def reference(orbitals, projectors, coupling, species, offsets):
    total_proj = projectors.shape[0]
    total_bands = orbitals.shape[0]
    per_atom = coupling.shape[1]
    flat_proj = projectors.reshape(total_proj, -1)
    turned = jnp.concatenate([orbitals[:, 1, :], -orbitals[:, 0, :]], axis=1)
    stacked = jnp.concatenate([orbitals.reshape(total_bands, -1), turned], axis=0)
    becp = lax.dot_general(flat_proj, stacked, (((1,), (1,)), ((), ())), preferred_element_type=jnp.float32)
    becp = becp.reshape(ATOMS, per_atom, 2 * total_bands)
    blocks = (offsets // per_atom).astype(jnp.int32)
    atom_kind = jnp.zeros((ATOMS,), jnp.int32).at[blocks].set(species)
    matrices = coupling[atom_kind].astype(jnp.float32)
    dbecp = jnp.einsum("aij,ajc->aic", matrices, becp, precision=lax.Precision.HIGHEST)
    dbecp = dbecp.reshape(total_proj, 2 * total_bands).astype(jnp.bfloat16)
    real_part = lax.dot_general(dbecp, projectors[:, 0, :], (((0,), (0,)), ((), ())), preferred_element_type=jnp.float32)
    imag_part = lax.dot_general(dbecp, projectors[:, 1, :], (((0,), (0,)), ((), ())), preferred_element_type=jnp.float32)
    out_real = real_part[:total_bands] - imag_part[total_bands:]
    out_imag = imag_part[:total_bands] + real_part[total_bands:]
    return jnp.stack([out_real, out_imag], axis=1).astype(jnp.bfloat16)
```

```python
import functools

import jax
import jax.numpy as jnp
import numpy as np
from jax import lax
from jax.experimental import pallas as pl
from jax.experimental.pallas import tpu as pltpu
from jax.sharding import PartitionSpec as P

MESH = pl.DeviceIdType.MESH
PLANE = 4
LINE = 4
TILE = 8
LANES = 128
F32 = jnp.float32
BF16 = jnp.bfloat16


def coupling_rows(coupling, species, offsets, total_proj):
    kinds, per_atom = coupling.shape[0], coupling.shape[1]
    column = jnp.arange(total_proj, dtype=jnp.int32)
    within = column % per_atom
    start = column - within
    kind = jnp.sum(
        jnp.where(offsets[:, None] == start[None, :], species[:, None], 0), axis=0
    )
    pick = (jnp.arange(kinds * per_atom, dtype=jnp.int32)[:, None] == (kind * per_atom + within)[None, :])
    table = jnp.transpose(coupling, (2, 0, 1)).reshape(per_atom, kinds * per_atom)
    return jnp.dot(table, pick.astype(F32), precision=lax.Precision.HIGHEST, preferred_element_type=F32)


def block_diagonal(rows, spread, start_col, start_row):
    full = lax.dot_general(
        spread, rows, (((1,), (0,)), ((), ())), precision=lax.Precision.HIGHEST, preferred_element_type=F32
    )
    return jnp.where(start_col == start_row, full, 0.0)


def block_maps(count, per_atom):
    index = np.arange(count)
    spread = (index[:, None] % per_atom == np.arange(per_atom)[None, :]).astype(np.float32)
    start = (index // per_atom).astype(np.int32)
    return spread, start[:, None], start[None, :]


def dot_t(a, b):
    return lax.dot_general(a, b, (((1,), (1,)), ((), ())), preferred_element_type=F32)


def dot(a, b):
    return lax.dot_general(a, b, (((1,), (0,)), ((), ())), preferred_element_type=F32)


def flip(bit, by):
    return bit + by - 2 * bit * by


def kernel(
    chunks, o_ref, p_ref, coupling_ref, species_ref, offsets_ref, out_ref,
    obuf, pbuf, coef, zbuf, psend, precv, total, zsend, zrecv, hsum, hsend, hrecv, dbuf, rbuf,
    f_send, f_recv, l_sem, t_send, t_recv, p_send, p_recv, z_send, z_recv, h_send, h_recv,
    e_send, e_recv, d_send, d_recv, r_send, r_recv,
):
    g = lax.axis_index("ga")
    me = lax.axis_index("band")
    proj, wide = p_ref.shape[1], p_ref.shape[2]
    height, width = zbuf.shape[1], zbuf.shape[2]
    unit = 2 * TILE
    members = height // unit
    quarter = height // PLANE
    half = quarter // 2
    per_atom = coupling_ref.shape[1]
    n, z = me % PLANE, me // PLANE
    x, y, z0, z1 = n % 2, n // 2, z % 2, z // 2

    def place(bx, by, b0, b1):
        return (b1 * 2 + b0) * PLANE + by * 2 + bx

    def slot(bx, by, b0, b1):
        return (by * 2 + bx) * LINE + b0 * 2 + b1

    def at(mask):
        bits = (flip(x, mask % 2), flip(y, (mask // 2) % 2), flip(z0, (mask // 4) % 2), flip(z1, mask // 8))
        return place(*bits), slot(*bits)

    my_slot = slot(x, y, z0, z1)
    twin = {"ga": 1 - g}
    plane = [(flip(x, j % 2), flip(y, j // 2)) for j in range(1, PLANE)]
    plane_at = [{"band": place(bx, by, z0, z1)} for bx, by in plane]
    near = {"band": place(x, y, 1 - z0, z1)}
    far = {"band": place(x, y, z0, 1 - z1)}

    def remote(src, dst, send, recv, to):
        return pltpu.make_async_remote_copy(
            src_ref=src, dst_ref=dst, send_sem=send, recv_sem=recv, device_id=to, device_id_type=MESH
        )

    barrier = pltpu.get_barrier_semaphore()
    pl.semaphore_signal(barrier, inc=1, device_id=twin, device_id_type=MESH)

    def greet(mask, carry):
        peer, _ = at(mask)
        for core in range(2):
            pl.semaphore_signal(barrier, inc=1, device_id={"ga": core, "band": peer}, device_id_type=MESH)
        return carry

    lax.fori_loop(1, members, greet, 0)

    def rows_of(i, core):
        return pl.ds(pl.multiple_of((i * 2 + core) * unit, unit), unit)

    def cols_of(index):
        return pl.ds(pl.multiple_of(index * wide, wide), wide)

    my_rows = pl.ds(pl.multiple_of(my_slot * unit, unit), unit)
    my_cols = cols_of(g)

    own_p = pltpu.make_async_copy(p_ref, pbuf.at[:, pl.ds(0, proj), my_cols], l_sem)
    own_p.start()
    for i in range(chunks):
        pltpu.make_async_copy(o_ref.at[rows_of(i, g), cols_of(me)], obuf.at[i, my_rows, my_cols], f_recv.at[i]).start()

    pl.semaphore_wait(barrier, 2 * members - 1)

    twin_p = remote(p_ref, pbuf.at[:, pl.ds(0, proj), my_cols], t_send, t_recv, twin)

    def f_copy(i, core, peer, to):
        return remote(
            o_ref.at[rows_of(i, core), cols_of(peer)], obuf.at[i, my_rows, my_cols], f_send.at[i], f_recv.at[i], to
        )

    def f_issue(i, first, last):
        def step(mask, carry):
            peer, _ = at(mask)
            for core in range(2):
                f_copy(i, core, peer, {"ga": core, "band": peer}).start()
            return carry

        lax.fori_loop(first, last, step, 0)

    def f_twin(i):
        f_copy(i, 1 - g, me, twin).start()

    def whole(ref, send, recv):
        return remote(ref, ref, send, recv, twin)

    def prepare():
        if width > proj:
            for c in range(2):
                pbuf[c, pl.ds(proj, width - proj), :] = jnp.zeros((width - proj, 2 * wide), BF16)
        column = lax.broadcasted_iota(jnp.int32, (offsets_ref.shape[0], width), 1)
        begin = offsets_ref[...]
        inside = (column >= begin) & (column < begin + per_atom)
        kind = jnp.sum(jnp.where(inside, species_ref[...], 0), axis=0, keepdims=True)
        start = jnp.sum(jnp.where(inside, begin, 0), axis=0, keepdims=True)
        within = lax.broadcasted_iota(jnp.int32, (1, width), 1) - start
        index = lax.broadcasted_iota(jnp.int32, (per_atom, width), 0)
        rows = jnp.zeros((per_atom, width), F32)
        for k in range(coupling_ref.shape[0]):
            pick = jnp.where((kind == k) & (within == index), 1.0, 0.0).astype(F32)
            rows = rows + lax.dot_general(
                coupling_ref[k], pick, (((0,), (0,)), ((), ())),
                precision=lax.Precision.HIGHEST, preferred_element_type=F32,
            )
        for s in range(1 - per_atom, per_atom):
            coef[pl.ds(s + per_atom - 1, 1), :] = jnp.sum(
                jnp.where(index == within - s, rows, 0.0), axis=0, keepdims=True
            )

    def piece(index, rows):
        return pl.ds(pl.multiple_of(index * rows, rows), rows)

    def blocks(count):
        step = 2 * LANES
        return [(low, min(step, count - low)) for low in range(0, count, step)]

    def split(value):
        return value.reshape(members, 2, TILE, value.shape[-1])

    def join(real, imag):
        return jnp.stack([real, imag], axis=1).reshape(height, real.shape[-1])

    pcopy, zcopy, hcopy, ecopy, dcopy = {}, {}, {}, {}, {}

    def project(i):
        whole(obuf.at[i], f_send.at[i], f_recv.at[i]).wait_recv()
        for low, size in blocks(width):
            a = split(dot_t(obuf[i], pbuf[0, pl.ds(low, size), :]))
            b = split(dot_t(obuf[i], pbuf[1, pl.ds(low, size), :]))
            zbuf[i, :, pl.ds(low, size)] = join(a[:, 0] + b[:, 1], a[:, 1] - b[:, 0])
        for j in range(PLANE - 1):
            bx, by = plane[j]
            psend[i, j] = zbuf[i, piece(by * 2 + bx, quarter), :].astype(BF16)
            pcopy[i, j] = remote(psend.at[i, j], precv.at[i, j], p_send.at[i, j], p_recv.at[i, j], plane_at[j])
            pcopy[i, j].start()

    def reduce_plane(i):
        value = zbuf[i, piece(n, quarter), :]
        for j in range(PLANE - 1):
            pcopy[i, j].wait_recv()
            value = value + precv[i, j].astype(F32)
        total[i] = value
        zsend[i] = total[i, piece(1 - z0, half), :].astype(BF16)
        zcopy[i] = remote(zsend.at[i], zrecv.at[i], z_send.at[i], z_recv.at[i], near)
        zcopy[i].start()

    def reduce_near(i):
        zcopy[i].wait_recv()
        value = total[i, piece(z0, half), :] + zrecv[i].astype(F32)
        hsum[i] = value
        hsend[i] = value.astype(BF16)
        hcopy[i] = remote(hsend.at[i], hrecv.at[i], h_send.at[i], h_recv.at[i], far)
        hcopy[i].start()

    def couple(i):
        hcopy[i].wait_recv()
        value = hsum[i] + hrecv[i].astype(F32)
        result = jnp.zeros_like(value)
        for s in range(1 - per_atom, per_atom):
            moved = value if s == 0 else pltpu.roll(value, s % width, 1)
            result = result + moved * coef[pl.ds(s + per_atom - 1, 1), :]
        mine = piece(n * 2 + z0, half)
        dbuf[i, mine, :] = result.astype(BF16)
        own = dbuf.at[i, mine, :]
        ecopy[i] = remote(own, own, e_send.at[i], e_recv.at[i], near)
        ecopy[i].start()
        for j in range(PLANE - 1):
            dcopy[i, 0, j] = remote(own, own, d_send.at[i, 0, j], d_recv.at[i, 0, j], plane_at[j])
            dcopy[i, 0, j].start()

    def hand_on(i):
        ecopy[i].wait_recv()
        got = dbuf.at[i, piece(n * 2 + 1 - z0, half), :]
        for j in range(PLANE - 1):
            dcopy[i, 1, j] = remote(got, got, d_send.at[i, 1, j], d_recv.at[i, 1, j], plane_at[j])
            dcopy[i, 1, j].start()

    def r_copy(i, there, core, to):
        rows = pl.ds(pl.multiple_of(there * unit, unit), unit)
        return remote(
            rbuf.at[i, rows, cols_of(core)], out_ref.at[rows_of(i, g), cols_of(me)], r_send.at[i], r_recv.at[i], to
        )

    def apply(i):
        for v in range(2):
            for j in range(PLANE - 1):
                dcopy[i, v, j].wait_recv()
        for low, size in blocks(2 * wide):
            a = split(dot(dbuf[i], pbuf[0, :, pl.ds(low, size)]))
            b = split(dot(dbuf[i], pbuf[1, :, pl.ds(low, size)]))
            rbuf[i, :, pl.ds(low, size)] = join(a[:, 0] - b[:, 1], b[:, 0] + a[:, 1]).astype(BF16)

        def step(mask, carry):
            peer, there = at(mask)
            for core in range(2):
                r_copy(i, there, core, {"ga": core, "band": peer}).start()
            return carry

        lax.fori_loop(1, members, step, 0)
        r_copy(i, my_slot, 1 - g, twin).start()
        pltpu.make_async_copy(
            rbuf.at[i, my_rows, cols_of(g)], out_ref.at[rows_of(i, g), cols_of(me)], r_recv.at[i]
        ).start()

    twin_p.start()
    f_twin(0)
    f_issue(0, 1, members)
    f_twin(1)
    f_issue(1, 1, members)
    prepare()
    own_p.wait()
    twin_p.wait_recv()

    for i in range(2, chunks):
        f_twin(i)
    project(0)
    f_issue(2, 1, members)
    reduce_plane(0)
    reduce_near(0)
    project(1)
    f_issue(3, 1, members)
    couple(0)
    reduce_plane(1)
    hand_on(0)
    reduce_near(1)
    project(2)
    apply(0)
    couple(1)
    reduce_plane(2)
    hand_on(1)
    reduce_near(2)
    project(3)
    apply(1)
    couple(2)
    reduce_plane(3)
    hand_on(2)
    reduce_near(3)
    apply(2)
    couple(3)
    hand_on(3)
    apply(3)

    twin_p.wait_send()
    for copies in (pcopy, zcopy, hcopy, ecopy, dcopy):
        for copy in copies.values():
            copy.wait_send()
    sent = pl.ds(0, height - unit // 2)
    for i in range(chunks):
        whole(obuf.at[i, sent, :], f_send.at[i], f_recv.at[i]).wait_send()
        whole(rbuf.at[i, sent, :], r_send.at[i], r_recv.at[i]).wait_send()
        whole(out_ref.at[pl.ds(i * 2 * unit, 2 * unit), :], r_send.at[i], r_recv.at[i]).wait_recv()


def fused(chunks, members, orbitals, projectors, coupling, species, offsets):
    rows, reach = orbitals.shape
    _, proj, wide = projectors.shape
    width = -(-proj // LANES) * LANES
    height = members * 2 * TILE
    quarter = height // PLANE
    half = quarter // 2
    per_atom = coupling.shape[1]
    taps = -(-(2 * per_atom - 1) // TILE) * TILE + TILE
    dma = pltpu.SemaphoreType.DMA
    hbm = pl.BlockSpec(memory_space=pl.ANY)
    flops = 32 * chunks * height * width * wide
    vm = pltpu.VMEM
    return pl.pallas_call(
        functools.partial(kernel, chunks),
        out_shape=jax.ShapeDtypeStruct((rows, reach), BF16),
        in_specs=[hbm, hbm] + [pl.BlockSpec(memory_space=pltpu.VMEM)] * 3,
        out_specs=hbm,
        scratch_shapes=[
            vm((chunks, height, 2 * wide), BF16),
            vm((2, width, 2 * wide), BF16),
            vm((taps, width), F32),
            vm((chunks, height, width), F32),
            vm((chunks, PLANE - 1, quarter, width), BF16),
            vm((chunks, PLANE - 1, quarter, width), BF16),
            vm((chunks, quarter, width), F32),
            vm((chunks, half, width), BF16),
            vm((chunks, half, width), BF16),
            vm((chunks, half, width), F32),
            vm((chunks, half, width), BF16),
            vm((chunks, half, width), BF16),
            vm((chunks, height, width), BF16),
            vm((chunks, height, 2 * wide), BF16),
            dma((chunks,)), dma((chunks,)), dma, dma, dma,
            dma((chunks, PLANE - 1)), dma((chunks, PLANE - 1)),
            dma((chunks,)), dma((chunks,)), dma((chunks,)), dma((chunks,)), dma((chunks,)), dma((chunks,)),
            dma((chunks, 2, PLANE - 1)), dma((chunks, 2, PLANE - 1)),
            dma((chunks,)), dma((chunks,)),
        ],
        compiler_params=pltpu.CompilerParams(
            collective_id=0, has_side_effects=True, vmem_limit_bytes=48 * 1024 * 1024
        ),
        cost_estimate=pl.CostEstimate(flops=flops, bytes_accessed=4 * rows * reach, transcendentals=0),
    )(orbitals, projectors, coupling, species, offsets)


def per_device_kernel(groups, members, orbitals, projectors, coupling, species, offsets):
    bands, _, reach = orbitals.shape
    blocks = bands // TILE
    turned = jnp.transpose(orbitals.reshape(blocks, TILE, 2, reach), (0, 2, 1, 3)).reshape(2 * bands, reach)
    result = fused(
        blocks // groups, members, turned, jnp.transpose(projectors, (1, 0, 2)), coupling,
        species[:, None], offsets[:, None],
    )
    return jnp.transpose(result.reshape(blocks, 2, TILE, reach), (0, 2, 1, 3)).reshape(bands, 2, reach)


def per_device_plain(orbitals, projectors, coupling, species, offsets):
    total_proj = projectors.shape[0]
    p_real, p_imag = projectors[:, 0, :], projectors[:, 1, :]
    rows = coupling_rows(coupling, species, offsets, total_proj)
    matrix = block_diagonal(rows, *block_maps(total_proj, coupling.shape[1]))
    spread = lax.all_to_all(orbitals, "band", split_axis=2, concat_axis=0, tiled=True)
    o_real, o_imag = spread[:, 0, :], spread[:, 1, :]
    partial_sum = jnp.stack(
        [dot_t(o_real, p_real) + dot_t(o_imag, p_imag), dot_t(o_imag, p_real) - dot_t(o_real, p_imag)], axis=1
    )
    becp = lax.psum_scatter(partial_sum, ("ga", "band"), scatter_dimension=0, tiled=True)
    coupled = jnp.einsum("bcp,pq->bcq", becp, matrix, precision=lax.Precision.HIGHEST).astype(BF16)
    dbecp = lax.all_gather(coupled, ("ga", "band"), axis=0, tiled=True)
    d_real, d_imag = dbecp[:, 0, :], dbecp[:, 1, :]
    result = jnp.stack(
        [dot(d_real, p_real) - dot(d_imag, p_imag), dot(d_real, p_imag) + dot(d_imag, p_real)], axis=1
    ).astype(BF16)
    return lax.all_to_all(result, "band", split_axis=0, concat_axis=2, tiled=True)


def solution(mesh):
    groups, members = mesh.shape["ga"], mesh.shape["band"]

    def body(orbitals, projectors, *rest):
        if groups == 2 and members == PLANE * LINE and orbitals.shape[0] == 4 * groups * TILE:
            return per_device_kernel(groups, members, orbitals, projectors, *rest)
        return per_device_plain(orbitals, projectors, *rest)

    placed = (P("band", None, "ga"), P(None, None, ("ga", "band")), P(), P(), P())
    return jax.shard_map(body, mesh=mesh, in_specs=placed, out_specs=P("band", None, "ga"), check_vma=False)
```

```python
import functools

import jax
import jax.numpy as jnp
import numpy as np
from jax import lax
from jax.experimental import pallas as pl
from jax.experimental.pallas import tpu as pltpu
from jax.sharding import PartitionSpec as P

MESH = pl.DeviceIdType.MESH
PLANE = 4
LINE = 4
TILE = 8
LANES = 128
F32 = jnp.float32
BF16 = jnp.bfloat16
VMEM_LIMIT = 63 * 1024 * 1024
WINDOW = 16
DELAYS = (12, 16, 20, 24, 28)


def coupling_rows(coupling, species, offsets, total_proj):
    kinds, per_atom = coupling.shape[0], coupling.shape[1]
    column = jnp.arange(total_proj, dtype=jnp.int32)
    within = column % per_atom
    start = column - within
    kind = jnp.sum(
        jnp.where(offsets[:, None] == start[None, :], species[:, None], 0), axis=0
    )
    pick = (jnp.arange(kinds * per_atom, dtype=jnp.int32)[:, None] == (kind * per_atom + within)[None, :])
    table = jnp.transpose(coupling, (2, 0, 1)).reshape(per_atom, kinds * per_atom)
    return jnp.dot(table, pick.astype(F32), precision=lax.Precision.HIGHEST, preferred_element_type=F32)


def block_diagonal(rows, spread, start_col, start_row):
    full = lax.dot_general(
        spread, rows, (((1,), (0,)), ((), ())), precision=lax.Precision.HIGHEST, preferred_element_type=F32
    )
    return jnp.where(start_col == start_row, full, 0.0)


def block_maps(count, per_atom):
    index = np.arange(count)
    spread = (index[:, None] % per_atom == np.arange(per_atom)[None, :]).astype(np.float32)
    start = (index // per_atom).astype(np.int32)
    return spread, start[:, None], start[None, :]


def dot_t(a, b):
    return lax.dot_general(a, b, (((1,), (1,)), ((), ())), preferred_element_type=F32)


def dot(a, b):
    return lax.dot_general(a, b, (((1,), (0,)), ((), ())), preferred_element_type=F32)


def flip(bit, by):
    return bit + by - 2 * bit * by


def kernel(
    chunks, o_ref, p_ref, coupling_ref, species_ref, offsets_ref, out_ref,
    obuf, praw, table, atoms, lbuf, pbuf, coef, zbuf, psend, precv, total, zsend, zrecv, hsum, hsend, hrecv, dbuf, rbuf,
    f_send, f_recv, l_sem, t_send, t_recv, p_send, p_recv, z_send, z_recv, h_send, h_recv,
    e_send, e_recv, d_send, d_recv, r_send, r_recv,
):
    g = lax.axis_index("ga")
    me = lax.axis_index("band")
    proj, wide = p_ref.shape[0], p_ref.shape[2]
    height, width = zbuf.shape[2], zbuf.shape[3]
    members = height // TILE
    quarter = height // PLANE
    half = quarter // 2
    per_atom = coupling_ref.shape[0]
    n, z = me % PLANE, me // PLANE
    x, y, z0, z1 = n % 2, n // 2, z % 2, z // 2

    def place(bx, by, b0, b1):
        return (b1 * 2 + b0) * PLANE + by * 2 + bx

    def slot(bx, by, b0, b1):
        return (by * 2 + bx) * LINE + b0 * 2 + b1

    def at(mask):
        bits = (flip(x, mask % 2), flip(y, (mask // 2) % 2), flip(z0, (mask // 4) % 2), flip(z1, mask // 8))
        return place(*bits), slot(*bits)

    my_slot = slot(x, y, z0, z1)
    twin = {"ga": 1 - g}
    plane = [(flip(x, j % 2), flip(y, j // 2)) for j in range(1, PLANE)]
    plane_at = [{"band": place(bx, by, z0, z1)} for bx, by in plane]
    near = {"band": place(x, y, 1 - z0, z1)}
    far = {"band": place(x, y, z0, 1 - z1)}
    peers = [None] + [at(mask) for mask in range(1, members)]

    def remote(src, dst, send, recv, to):
        return pltpu.make_async_remote_copy(
            src_ref=src, dst_ref=dst, send_sem=send, recv_sem=recv, device_id=to, device_id_type=MESH
        )

    barrier = pltpu.get_barrier_semaphore()
    pl.semaphore_signal(barrier, inc=1, device_id=twin, device_id_type=MESH)
    for mask in range(1, members):
        for core in range(2):
            pl.semaphore_signal(
                barrier, inc=1, device_id={"ga": core, "band": peers[mask][0]}, device_id_type=MESH
            )

    def piece(index, rows):
        return pl.ds(pl.multiple_of(index * rows, rows), rows)

    def rows_of(i, core):
        return piece(i * 2 + core, TILE)

    def cols_of(index):
        return piece(index, wide)

    my_rows = piece(my_slot, TILE)
    my_cols = cols_of(g)

    local = [
        pltpu.make_async_copy(p_ref, praw.at[g], l_sem.at[0]),
        pltpu.make_async_copy(coupling_ref, table, l_sem.at[1]),
        pltpu.make_async_copy(species_ref, atoms.at[0], l_sem.at[2]),
        pltpu.make_async_copy(offsets_ref, atoms.at[1], l_sem.at[3]),
    ]
    for copy in local:
        copy.start()
    for i in range(chunks):
        pltpu.make_async_copy(
            o_ref.at[rows_of(i, g), :, cols_of(me)], obuf.at[i, my_rows, :, my_cols], f_recv.at[i]
        ).start()

    pl.semaphore_wait(barrier, 2 * members - 1)

    twin_p = remote(p_ref, praw.at[g], t_send, t_recv, twin)

    def f_copy(i, q, core, peer, to, block=None):
        rows = rows_of(i, core if block is None else block)
        return remote(
            o_ref.at[rows, :, cols_of(peer)], obuf.at[i, my_rows, :, my_cols],
            f_send.at[i, q, core], f_recv.at[i], to,
        )

    def batch(q):
        inside = [q + 1] if q + 1 < PLANE else []
        return inside + [step * PLANE + q for step in range(1, members // PLANE)]

    def f_part(i, q, core):
        for mask in batch(q):
            peer, _ = peers[mask]
            f_copy(i, q, core, peer, {"ga": core, "band": peer}).start()

    def f_twin(i):
        f_copy(i, PLANE, 0, me, twin, 1 - g).start()

    def whole(ref, send, recv):
        return remote(ref, ref, send, recv, twin)

    def prepare():
        for copy in local:
            copy.wait()
        count = atoms.shape[2]
        turn = lax.broadcasted_iota(jnp.int32, (count, count), 0) == lax.broadcasted_iota(jnp.int32, (count, count), 1)

        def upright(row):
            return jnp.sum(jnp.where(turn, row.astype(F32), 0.0), axis=1, keepdims=True)

        column = lax.broadcasted_iota(jnp.int32, (count, width), 1).astype(F32)
        begin = upright(atoms[1])
        inside = (column >= begin) & (column < begin + per_atom)
        kind = jnp.sum(jnp.where(inside, upright(atoms[0]), 0.0), axis=0, keepdims=True)
        start = jnp.sum(jnp.where(inside, begin, 0.0), axis=0, keepdims=True)
        kind = (kind + 0.5).astype(jnp.int32)
        within = lax.broadcasted_iota(jnp.int32, (1, width), 1) - (start + 0.5).astype(jnp.int32)
        index = lax.broadcasted_iota(jnp.int32, (per_atom, width), 0)
        rows = jnp.zeros((per_atom, width), F32)
        for k in range(coupling_ref.shape[1]):
            pick = jnp.where((kind == k) & (within == index), 1.0, 0.0).astype(F32)
            rows = rows + lax.dot_general(
                table[:, k, :], pick, (((0,), (0,)), ((), ())),
                precision=lax.Precision.HIGHEST, preferred_element_type=F32,
            )
        for s in range(1 - per_atom, per_atom):
            coef[pl.ds(s + per_atom - 1, 1), :] = jnp.sum(
                jnp.where(index == within - s, rows, 0.0), axis=0, keepdims=True
            )
        twin_p.wait_recv()
        for c in range(2):
            for core in range(2):
                cols = pl.ds(core * wide, wide)
                if width > proj:
                    pbuf[c, pl.ds(proj, width - proj), cols] = jnp.zeros((width - proj, wide), BF16)

        def unpack(r, carry):
            rows = piece(r, 2 * TILE)
            for core in range(2):
                pbuf[:, rows, pl.ds(core * wide, wide)] = jnp.swapaxes(praw[core, rows], 0, 1)
            return carry

        lax.fori_loop(0, proj // (2 * TILE), unpack, 0)

    def blocks(count):
        step = 2 * LANES
        return [(low, min(step, count - low)) for low in range(0, count, step)]

    pcopy, zcopy, hcopy, ecopy, dcopy = {}, {}, {}, {}, {}

    def project(i):
        whole(obuf.at[i], f_send.at[i, 0, 0], f_recv.at[i]).wait_recv()
        for r in range(0, height, 2 * TILE):
            lbuf[:, pl.ds(r, 2 * TILE), :] = jnp.swapaxes(obuf[i, pl.ds(r, 2 * TILE)], 0, 1)
        left = lbuf[...].reshape(2 * height, 2 * wide)
        for low, size in blocks(width):
            a = dot_t(left, pbuf[0, pl.ds(low, size), :])
            b = dot_t(left, pbuf[1, pl.ds(low, size), :])
            zbuf[i, 0, :, pl.ds(low, size)] = a[:height] + b[height:]
            zbuf[i, 1, :, pl.ds(low, size)] = a[height:] - b[:height]
        for j in range(PLANE - 1):
            bx, by = plane[j]
            psend[i, j] = zbuf[i, :, piece(by * 2 + bx, quarter), :].astype(BF16)
            pcopy[i, j] = remote(psend.at[i, j], precv.at[i, j], p_send.at[i, j], p_recv.at[i, j], plane_at[j])
            pcopy[i, j].start()

    def reduce_plane(i):
        value = zbuf[i, :, piece(n, quarter), :]
        for j in range(PLANE - 1):
            pcopy[i, j].wait_recv()
            value = value + precv[i, j].astype(F32)
        total[i] = value
        zsend[i] = total[i, :, piece(1 - z0, half), :].astype(BF16)
        zcopy[i] = remote(zsend.at[i], zrecv.at[i], z_send.at[i], z_recv.at[i], near)
        zcopy[i].start()

    def reduce_near(i):
        zcopy[i].wait_recv()
        value = total[i, :, piece(z0, half), :] + zrecv[i].astype(F32)
        hsum[i] = value
        hsend[i] = value.astype(BF16)
        hcopy[i] = remote(hsend.at[i], hrecv.at[i], h_send.at[i], h_recv.at[i], far)
        hcopy[i].start()

    def couple(i):
        hcopy[i].wait_recv()
        value = (hsum[i] + hrecv[i].astype(F32)).reshape(2 * half, width)
        result = jnp.zeros_like(value)
        for s in range(1 - per_atom, per_atom):
            moved = value if s == 0 else pltpu.roll(value, s % width, 1)
            result = result + moved * coef[pl.ds(s + per_atom - 1, 1), :]
        mine = piece(n * 2 + z0, half)
        dbuf[i, :, mine, :] = result.astype(BF16).reshape(2, half, width)
        own = dbuf.at[i, :, mine, :]
        ecopy[i] = remote(own, own, e_send.at[i], e_recv.at[i], near)
        ecopy[i].start()
        for j in range(PLANE - 1):
            dcopy[i, 0, j] = remote(own, own, d_send.at[i, 0, j], d_recv.at[i, 0, j], plane_at[j])
            dcopy[i, 0, j].start()

    def hand_on(i):
        ecopy[i].wait_recv()
        got = dbuf.at[i, :, piece(n * 2 + 1 - z0, half), :]
        for j in range(PLANE - 1):
            dcopy[i, 1, j] = remote(got, got, d_send.at[i, 1, j], d_recv.at[i, 1, j], plane_at[j])
            dcopy[i, 1, j].start()

    def r_copy(i, q, core, there, to, block=None):
        return remote(
            rbuf.at[i, piece(there, TILE), :, cols_of(core if block is None else block)],
            out_ref.at[rows_of(i, g), :, cols_of(me)], r_send.at[i, q, core], r_recv.at[i], to,
        )

    def r_part(i, q, core):
        for mask in batch(q):
            peer, there = peers[mask]
            r_copy(i, q, core, there, {"ga": core, "band": peer}).start()

    def sent(k):
        phase, i, q, core = batches[k]
        ref = (obuf, rbuf)[phase].at[i, pl.ds(0, len(batch(q)) * TILE // 2)]
        send = (f_send, r_send)[phase].at[i, q, core]
        whole(ref, send, (f_recv, r_recv)[phase].at[i]).wait_send()

    def apply(i, core):
        if core == 0:
            for v in range(2):
                for j in range(PLANE - 1):
                    dcopy[i, v, j].wait_recv()
        left = dbuf[i].reshape(2 * height, width)
        for low, size in blocks(wide):
            cols = pl.ds(core * wide + low, size)
            a = dot(left, pbuf[0, :, cols])
            b = dot(left, pbuf[1, :, cols])
            both = jnp.stack([a[:height] - b[height:], b[:height] + a[height:]]).astype(BF16)
            for r in range(0, height, 2 * TILE):
                rbuf[i, pl.ds(r, 2 * TILE), :, cols] = jnp.swapaxes(both[:, r : r + 2 * TILE], 0, 1)
        if core == 1:
            r_copy(i, PLANE, 0, my_slot, twin, 1 - g).start()
            pltpu.make_async_copy(
                rbuf.at[i, my_rows, :, cols_of(g)], out_ref.at[rows_of(i, g), :, cols_of(me)], r_recv.at[i]
            ).start()

    batches = [
        (phase, i, q, core)
        for phase in range(2) for i in range(chunks) for core in range(2) for q in range(PLANE)
    ]
    each = 2 * PLANE
    stages = (project, reduce_plane, reduce_near, couple, hand_on)
    plan = {}
    for i in range(chunks):
        for stage, delay in zip(stages, DELAYS):
            plan.setdefault(min(i * each + delay, len(batches) // 2 + i * each), []).append((stage, i))

    twin_p.start()
    for k, (phase, i, q, core) in enumerate(batches):
        for stage, index in sorted(plan.get(k, []), key=lambda item: item[1]):
            stage(index)
        if k == each // 2:
            prepare()
        if k >= WINDOW:
            sent(k - WINDOW)
        if phase:
            if q == 0:
                apply(i, core)
            r_part(i, q, core)
        else:
            if core + q == 0:
                f_twin(i)
            f_part(i, q, core)

    for k in range(len(batches) - WINDOW, len(batches)):
        sent(k)
    twin_p.wait_send()
    for copies in (pcopy, zcopy, hcopy, ecopy, dcopy):
        for copy in copies.values():
            copy.wait_send()
    single = pl.ds(0, TILE // 2)
    for i in range(chunks):
        whole(obuf.at[i, single], f_send.at[i, PLANE, 0], f_recv.at[i]).wait_send()
        whole(rbuf.at[i, single], r_send.at[i, PLANE, 0], r_recv.at[i]).wait_send()
        whole(out_ref.at[pl.ds(i * 2 * TILE, 2 * TILE)], r_send.at[i, PLANE, 0], r_recv.at[i]).wait_recv()


def fused(chunks, members, orbitals, projectors, coupling, species, offsets):
    bands, _, reach = orbitals.shape
    proj, _, wide = projectors.shape
    width = -(-proj // LANES) * LANES
    height = members * TILE
    quarter = height // PLANE
    half = quarter // 2
    per_atom = coupling.shape[0]
    taps = -(-(2 * per_atom - 1) // TILE) * TILE + TILE
    dma = pltpu.SemaphoreType.DMA
    hbm = pl.BlockSpec(memory_space=pl.ANY)
    flops = 64 * chunks * height * width * wide
    vm = pltpu.VMEM
    steps = dma((chunks,))
    return pl.pallas_call(
        functools.partial(kernel, chunks),
        out_shape=jax.ShapeDtypeStruct(orbitals.shape, BF16),
        in_specs=[hbm] * 5,
        out_specs=hbm,
        scratch_shapes=[
            vm((chunks, height, 2, 2 * wide), BF16),
            vm((2, proj, 2, wide), BF16),
            vm(coupling.shape, F32),
            vm((2,) + species.shape, jnp.int32),
            vm((2, height, 2 * wide), BF16),
            vm((2, width, 2 * wide), BF16),
            vm((taps, width), F32),
            vm((chunks, 2, height, width), F32),
            vm((chunks, PLANE - 1, 2, quarter, width), BF16),
            vm((chunks, PLANE - 1, 2, quarter, width), BF16),
            vm((chunks, 2, quarter, width), F32),
            vm((chunks, 2, half, width), BF16),
            vm((chunks, 2, half, width), BF16),
            vm((chunks, 2, half, width), F32),
            vm((chunks, 2, half, width), BF16),
            vm((chunks, 2, half, width), BF16),
            vm((chunks, 2, height, width), BF16),
            vm((chunks, height, 2, 2 * wide), BF16),
            dma((chunks, PLANE + 1, 2)), steps, dma((4,)), dma, dma,
            dma((chunks, PLANE - 1)), dma((chunks, PLANE - 1)),
            steps, steps, steps, steps, steps, steps,
            dma((chunks, 2, PLANE - 1)), dma((chunks, 2, PLANE - 1)),
            dma((chunks, PLANE + 1, 2)), steps,
        ],
        compiler_params=pltpu.CompilerParams(
            collective_id=0, has_side_effects=True, vmem_limit_bytes=VMEM_LIMIT
        ),
        cost_estimate=pl.CostEstimate(flops=flops, bytes_accessed=8 * bands * reach, transcendentals=0),
    )(orbitals, projectors, coupling, species, offsets)


def per_device_kernel(groups, members, orbitals, projectors, coupling, species, offsets):
    chunks = orbitals.shape[0] // (groups * TILE)
    return fused(
        chunks, members, orbitals, projectors, jnp.transpose(coupling, (1, 0, 2)), species[None, :], offsets[None, :]
    )


def per_device_plain(orbitals, projectors, coupling, species, offsets):
    total_proj = projectors.shape[0]
    p_real, p_imag = projectors[:, 0, :], projectors[:, 1, :]
    rows = coupling_rows(coupling, species, offsets, total_proj)
    matrix = block_diagonal(rows, *block_maps(total_proj, coupling.shape[1]))
    spread = lax.all_to_all(orbitals, "band", split_axis=2, concat_axis=0, tiled=True)
    o_real, o_imag = spread[:, 0, :], spread[:, 1, :]
    partial_sum = jnp.stack(
        [dot_t(o_real, p_real) + dot_t(o_imag, p_imag), dot_t(o_imag, p_real) - dot_t(o_real, p_imag)], axis=1
    )
    becp = lax.psum_scatter(partial_sum, ("ga", "band"), scatter_dimension=0, tiled=True)
    coupled = jnp.einsum("bcp,pq->bcq", becp, matrix, precision=lax.Precision.HIGHEST).astype(BF16)
    dbecp = lax.all_gather(coupled, ("ga", "band"), axis=0, tiled=True)
    d_real, d_imag = dbecp[:, 0, :], dbecp[:, 1, :]
    result = jnp.stack(
        [dot(d_real, p_real) - dot(d_imag, p_imag), dot(d_real, p_imag) + dot(d_imag, p_real)], axis=1
    ).astype(BF16)
    return lax.all_to_all(result, "band", split_axis=0, concat_axis=2, tiled=True)


def solution(mesh):
    groups, members = mesh.shape["ga"], mesh.shape["band"]

    def body(orbitals, projectors, *rest):
        fits = orbitals.shape[0] % (groups * TILE) == 0 and projectors.shape[0] % (2 * TILE) == 0
        if groups == 2 and members == PLANE * LINE and fits:
            return per_device_kernel(groups, members, orbitals, projectors, *rest)
        return per_device_plain(orbitals, projectors, *rest)

    placed = (P("band", None, "ga"), P(None, None, ("ga", "band")), P(), P(), P())
    return jax.shard_map(body, mesh=mesh, in_specs=placed, out_specs=P("band", None, "ga"), check_vma=False)
```

```python
import functools

import jax
import jax.numpy as jnp
import numpy as np
from jax import lax
from jax.experimental import pallas as pl
from jax.experimental.pallas import tpu as pltpu
from jax.sharding import PartitionSpec as P

MESH = pl.DeviceIdType.MESH
PLANE = 4
LINE = 4
TILE = 8
LANES = 128
F32 = jnp.float32
BF16 = jnp.bfloat16
VMEM_LIMIT = 63 * 1024 * 1024
WINDOW = 64
DELAYS = (
    (12, 16, 20, 24, 28),
    (12, 16, 20, 24, 28),
    (12, 16, 20, 24, 28),
    (12, 17, 20, 24, 28),
)


def coupling_rows(coupling, species, offsets, total_proj):
    kinds, per_atom = coupling.shape[0], coupling.shape[1]
    column = jnp.arange(total_proj, dtype=jnp.int32)
    within = column % per_atom
    start = column - within
    kind = jnp.sum(
        jnp.where(offsets[:, None] == start[None, :], species[:, None], 0), axis=0
    )
    pick = (jnp.arange(kinds * per_atom, dtype=jnp.int32)[:, None] == (kind * per_atom + within)[None, :])
    table = jnp.transpose(coupling, (2, 0, 1)).reshape(per_atom, kinds * per_atom)
    return jnp.dot(table, pick.astype(F32), precision=lax.Precision.HIGHEST, preferred_element_type=F32)


def block_diagonal(rows, spread, start_col, start_row):
    full = lax.dot_general(
        spread, rows, (((1,), (0,)), ((), ())), precision=lax.Precision.HIGHEST, preferred_element_type=F32
    )
    return jnp.where(start_col == start_row, full, 0.0)


def block_maps(count, per_atom):
    index = np.arange(count)
    spread = (index[:, None] % per_atom == np.arange(per_atom)[None, :]).astype(np.float32)
    start = (index // per_atom).astype(np.int32)
    return spread, start[:, None], start[None, :]


def dot_t(a, b):
    return lax.dot_general(a, b, (((1,), (1,)), ((), ())), preferred_element_type=F32)


def dot(a, b):
    return lax.dot_general(a, b, (((1,), (0,)), ((), ())), preferred_element_type=F32)


def flip(bit, by):
    return bit + by - 2 * bit * by


def kernel(
    chunks, o_ref, p_ref, coupling_ref, species_ref, offsets_ref, out_ref,
    obuf, praw, table, atoms, lbuf, pbuf, coef, zbuf, psend, precv, total, zsend, zrecv, hsum, hsend, hrecv, dbuf, rbuf,
    f_send, f_recv, l_sem, t_send, t_recv, p_send, p_recv, z_send, z_recv, h_send, h_recv,
    e_send, e_recv, d_send, d_recv, r_send, r_recv,
):
    g = lax.axis_index("ga")
    me = lax.axis_index("band")
    proj, wide = p_ref.shape[0], p_ref.shape[2]
    height, width = zbuf.shape[2], zbuf.shape[3]
    members = height // TILE
    quarter = height // PLANE
    half = quarter // 2
    per_atom = coupling_ref.shape[0]
    n, z = me % PLANE, me // PLANE
    x, y, z0, z1 = n % 2, n // 2, z % 2, z // 2

    def place(bx, by, b0, b1):
        return (b1 * 2 + b0) * PLANE + by * 2 + bx

    def slot(bx, by, b0, b1):
        return (by * 2 + bx) * LINE + b0 * 2 + b1

    def at(mask):
        bits = (flip(x, mask % 2), flip(y, (mask // 2) % 2), flip(z0, (mask // 4) % 2), flip(z1, mask // 8))
        return place(*bits), slot(*bits)

    my_slot = slot(x, y, z0, z1)
    twin = {"ga": 1 - g}
    plane = [(flip(x, j % 2), flip(y, j // 2)) for j in range(1, PLANE)]
    plane_at = [{"band": place(bx, by, z0, z1)} for bx, by in plane]
    near = {"band": place(x, y, 1 - z0, z1)}
    far = {"band": place(x, y, z0, 1 - z1)}
    peers = [None] + [at(mask) for mask in range(1, members)]

    def remote(src, dst, send, recv, to):
        return pltpu.make_async_remote_copy(
            src_ref=src, dst_ref=dst, send_sem=send, recv_sem=recv, device_id=to, device_id_type=MESH
        )

    barrier = pltpu.get_barrier_semaphore()
    pl.semaphore_signal(barrier, inc=1, device_id=twin, device_id_type=MESH)
    for mask in range(1, members):
        for core in range(2):
            pl.semaphore_signal(
                barrier, inc=1, device_id={"ga": core, "band": peers[mask][0]}, device_id_type=MESH
            )

    def piece(index, rows):
        return pl.ds(pl.multiple_of(index * rows, rows), rows)

    def rows_of(i, core):
        return piece(i * 2 + core, TILE)

    def cols_of(index):
        return piece(index, wide)

    my_rows = piece(my_slot, TILE)
    my_cols = cols_of(g)

    local = [
        pltpu.make_async_copy(p_ref, praw.at[g], l_sem.at[0]),
        pltpu.make_async_copy(coupling_ref, table, l_sem.at[1]),
        pltpu.make_async_copy(species_ref, atoms.at[0], l_sem.at[2]),
        pltpu.make_async_copy(offsets_ref, atoms.at[1], l_sem.at[3]),
    ]
    for copy in local:
        copy.start()
    for i in range(chunks):
        pltpu.make_async_copy(
            o_ref.at[rows_of(i, g), :, cols_of(me)], obuf.at[i, my_rows, :, my_cols], f_recv.at[i]
        ).start()

    pl.semaphore_wait(barrier, 2 * members - 1)

    twin_p = remote(p_ref, praw.at[g], t_send, t_recv, twin)

    def f_copy(i, q, core, peer, to, block=None):
        rows = rows_of(i, core if block is None else block)
        return remote(
            o_ref.at[rows, :, cols_of(peer)], obuf.at[i, my_rows, :, my_cols],
            f_send.at[i, q, core], f_recv.at[i], to,
        )

    def batch(q):
        inside = [q + 1] if q + 1 < PLANE else []
        return inside + [step * PLANE + q for step in range(1, members // PLANE)]

    def f_part(i, q, core):
        for mask in batch(q):
            peer, _ = peers[mask]
            f_copy(i, q, core, peer, {"ga": core, "band": peer}).start()

    def f_twin(i):
        f_copy(i, PLANE, 0, me, twin, 1 - g).start()

    def whole(ref, send, recv):
        return remote(ref, ref, send, recv, twin)

    def prepare():
        for copy in local:
            copy.wait()
        count = atoms.shape[2]
        turn = lax.broadcasted_iota(jnp.int32, (count, count), 0) == lax.broadcasted_iota(jnp.int32, (count, count), 1)

        def upright(row):
            return jnp.sum(jnp.where(turn, row.astype(F32), 0.0), axis=1, keepdims=True)

        column = lax.broadcasted_iota(jnp.int32, (count, width), 1).astype(F32)
        begin = upright(atoms[1])
        inside = (column >= begin) & (column < begin + per_atom)
        kind = jnp.sum(jnp.where(inside, upright(atoms[0]), 0.0), axis=0, keepdims=True)
        start = jnp.sum(jnp.where(inside, begin, 0.0), axis=0, keepdims=True)
        kind = (kind + 0.5).astype(jnp.int32)
        within = lax.broadcasted_iota(jnp.int32, (1, width), 1) - (start + 0.5).astype(jnp.int32)
        index = lax.broadcasted_iota(jnp.int32, (per_atom, width), 0)
        rows = jnp.zeros((per_atom, width), F32)
        for k in range(coupling_ref.shape[1]):
            pick = jnp.where((kind == k) & (within == index), 1.0, 0.0).astype(F32)
            rows = rows + lax.dot_general(
                table[:, k, :], pick, (((0,), (0,)), ((), ())),
                precision=lax.Precision.HIGHEST, preferred_element_type=F32,
            )
        for s in range(1 - per_atom, per_atom):
            coef[pl.ds(s + per_atom - 1, 1), :] = jnp.sum(
                jnp.where(index == within - s, rows, 0.0), axis=0, keepdims=True
            )
        twin_p.wait_recv()
        for c in range(2):
            for core in range(2):
                cols = pl.ds(core * wide, wide)
                if width > proj:
                    pbuf[c, pl.ds(proj, width - proj), cols] = jnp.zeros((width - proj, wide), BF16)

        def unpack(r, carry):
            rows = piece(r, 2 * TILE)
            for core in range(2):
                pbuf[:, rows, pl.ds(core * wide, wide)] = jnp.swapaxes(praw[core, rows], 0, 1)
            return carry

        lax.fori_loop(0, proj // (2 * TILE), unpack, 0)

    def blocks(count):
        step = 2 * LANES
        return [(low, min(step, count - low)) for low in range(0, count, step)]

    pcopy, zcopy, hcopy, ecopy, dcopy = {}, {}, {}, {}, {}

    def project(i):
        whole(obuf.at[i], f_send.at[i, 0, 0], f_recv.at[i]).wait_recv()
        for r in range(0, height, 2 * TILE):
            lbuf[:, pl.ds(r, 2 * TILE), :] = jnp.swapaxes(obuf[i, pl.ds(r, 2 * TILE)], 0, 1)
        left = lbuf[...].reshape(2 * height, 2 * wide)
        for low, size in blocks(width):
            a = dot_t(left, pbuf[0, pl.ds(low, size), :])
            b = dot_t(left, pbuf[1, pl.ds(low, size), :])
            zbuf[i, 0, :, pl.ds(low, size)] = a[:height] + b[height:]
            zbuf[i, 1, :, pl.ds(low, size)] = a[height:] - b[:height]
        for j in range(PLANE - 1):
            bx, by = plane[j]
            psend[i, j] = zbuf[i, :, piece(by * 2 + bx, quarter), :].astype(BF16)
            pcopy[i, j] = remote(psend.at[i, j], precv.at[i, j], p_send.at[i, j], p_recv.at[i, j], plane_at[j])
            pcopy[i, j].start()

    def reduce_plane(i):
        value = zbuf[i, :, piece(n, quarter), :]
        for j in range(PLANE - 1):
            pcopy[i, j].wait_recv()
            value = value + precv[i, j].astype(F32)
        total[i] = value
        zsend[i] = total[i, :, piece(1 - z0, half), :].astype(BF16)
        zcopy[i] = remote(zsend.at[i], zrecv.at[i], z_send.at[i], z_recv.at[i], near)
        zcopy[i].start()

    def reduce_near(i):
        zcopy[i].wait_recv()
        value = total[i, :, piece(z0, half), :] + zrecv[i].astype(F32)
        hsum[i] = value
        hsend[i] = value.astype(BF16)
        hcopy[i] = remote(hsend.at[i], hrecv.at[i], h_send.at[i], h_recv.at[i], far)
        hcopy[i].start()

    def couple(i):
        hcopy[i].wait_recv()
        value = (hsum[i] + hrecv[i].astype(F32)).reshape(2 * half, width)
        result = jnp.zeros_like(value)
        for s in range(1 - per_atom, per_atom):
            moved = value if s == 0 else pltpu.roll(value, s % width, 1)
            result = result + moved * coef[pl.ds(s + per_atom - 1, 1), :]
        mine = piece(n * 2 + z0, half)
        dbuf[i, :, mine, :] = result.astype(BF16).reshape(2, half, width)
        own = dbuf.at[i, :, mine, :]
        ecopy[i] = remote(own, own, e_send.at[i], e_recv.at[i], near)
        ecopy[i].start()
        for j in range(PLANE - 1):
            dcopy[i, 0, j] = remote(own, own, d_send.at[i, 0, j], d_recv.at[i, 0, j], plane_at[j])
            dcopy[i, 0, j].start()

    def hand_on(i):
        ecopy[i].wait_recv()
        got = dbuf.at[i, :, piece(n * 2 + 1 - z0, half), :]
        for j in range(PLANE - 1):
            dcopy[i, 1, j] = remote(got, got, d_send.at[i, 1, j], d_recv.at[i, 1, j], plane_at[j])
            dcopy[i, 1, j].start()

    def r_copy(i, q, core, there, to, block=None):
        return remote(
            rbuf.at[i, piece(there, TILE), :, cols_of(core if block is None else block)],
            out_ref.at[rows_of(i, g), :, cols_of(me)], r_send.at[i, q, core], r_recv.at[i], to,
        )

    def r_part(i, q, core):
        for mask in batch(q):
            peer, there = peers[mask]
            r_copy(i, q, core, there, {"ga": core, "band": peer}).start()

    def sent(k):
        phase, i, q, core = batches[k]
        ref = (obuf, rbuf)[phase].at[i, pl.ds(0, len(batch(q)) * TILE // 2)]
        send = (f_send, r_send)[phase].at[i, q, core]
        whole(ref, send, (f_recv, r_recv)[phase].at[i]).wait_send()

    def apply(i, core):
        if core == 0:
            for v in range(2):
                for j in range(PLANE - 1):
                    dcopy[i, v, j].wait_recv()
        left = dbuf[i].reshape(2 * height, width)
        for low, size in blocks(wide):
            cols = pl.ds(core * wide + low, size)
            a = dot(left, pbuf[0, :, cols])
            b = dot(left, pbuf[1, :, cols])
            both = jnp.stack([a[:height] - b[height:], b[:height] + a[height:]]).astype(BF16)
            for r in range(0, height, 2 * TILE):
                rbuf[i, pl.ds(r, 2 * TILE), :, cols] = jnp.swapaxes(both[:, r : r + 2 * TILE], 0, 1)
        if core == 1:
            r_copy(i, PLANE, 0, my_slot, twin, 1 - g).start()
            pltpu.make_async_copy(
                rbuf.at[i, my_rows, :, cols_of(g)], out_ref.at[rows_of(i, g), :, cols_of(me)], r_recv.at[i]
            ).start()

    batches = [
        (phase, i, q, core)
        for phase in range(2) for i in range(chunks) for core in range(2) for q in range(PLANE)
    ]
    each = 2 * PLANE
    stages = (project, reduce_plane, reduce_near, couple, hand_on)
    plan = {}
    for i in range(chunks):
        for stage, delay in zip(stages, DELAYS[min(i, len(DELAYS) - 1)]):
            plan.setdefault(min(i * each + delay, len(batches) // 2 + i * each), []).append((stage, i))

    twin_p.start()
    for k, (phase, i, q, core) in enumerate(batches):
        for stage, index in sorted(plan.get(k, []), key=lambda item: item[1]):
            stage(index)
        if k == each // 2:
            prepare()
        if k >= WINDOW:
            sent(k - WINDOW)
        if phase:
            if q == 0:
                apply(i, core)
            r_part(i, q, core)
        else:
            if core + q == 0:
                f_twin(i)
            f_part(i, q, core)

    for k in range(max(len(batches) - WINDOW, 0), len(batches)):
        sent(k)
    twin_p.wait_send()
    for copies in (pcopy, zcopy, hcopy, ecopy, dcopy):
        for copy in copies.values():
            copy.wait_send()
    single = pl.ds(0, TILE // 2)
    for i in range(chunks):
        whole(obuf.at[i, single], f_send.at[i, PLANE, 0], f_recv.at[i]).wait_send()
        whole(rbuf.at[i, single], r_send.at[i, PLANE, 0], r_recv.at[i]).wait_send()
        whole(out_ref.at[pl.ds(i * 2 * TILE, 2 * TILE)], r_send.at[i, PLANE, 0], r_recv.at[i]).wait_recv()


def fused(chunks, members, orbitals, projectors, coupling, species, offsets):
    bands, _, reach = orbitals.shape
    proj, _, wide = projectors.shape
    width = -(-proj // LANES) * LANES
    height = members * TILE
    quarter = height // PLANE
    half = quarter // 2
    per_atom = coupling.shape[0]
    taps = -(-(2 * per_atom - 1) // TILE) * TILE + TILE
    dma = pltpu.SemaphoreType.DMA
    hbm = pl.BlockSpec(memory_space=pl.ANY)
    flops = 64 * chunks * height * width * wide
    vm = pltpu.VMEM
    steps = dma((chunks,))
    return pl.pallas_call(
        functools.partial(kernel, chunks),
        out_shape=jax.ShapeDtypeStruct(orbitals.shape, BF16),
        in_specs=[hbm] * 5,
        out_specs=hbm,
        scratch_shapes=[
            vm((chunks, height, 2, 2 * wide), BF16),
            vm((2, proj, 2, wide), BF16),
            vm(coupling.shape, F32),
            vm((2,) + species.shape, jnp.int32),
            vm((2, height, 2 * wide), BF16),
            vm((2, width, 2 * wide), BF16),
            vm((taps, width), F32),
            vm((chunks, 2, height, width), F32),
            vm((chunks, PLANE - 1, 2, quarter, width), BF16),
            vm((chunks, PLANE - 1, 2, quarter, width), BF16),
            vm((chunks, 2, quarter, width), F32),
            vm((chunks, 2, half, width), BF16),
            vm((chunks, 2, half, width), BF16),
            vm((chunks, 2, half, width), F32),
            vm((chunks, 2, half, width), BF16),
            vm((chunks, 2, half, width), BF16),
            vm((chunks, 2, height, width), BF16),
            vm((chunks, height, 2, 2 * wide), BF16),
            dma((chunks, PLANE + 1, 2)), steps, dma((4,)), dma, dma,
            dma((chunks, PLANE - 1)), dma((chunks, PLANE - 1)),
            steps, steps, steps, steps, steps, steps,
            dma((chunks, 2, PLANE - 1)), dma((chunks, 2, PLANE - 1)),
            dma((chunks, PLANE + 1, 2)), steps,
        ],
        compiler_params=pltpu.CompilerParams(
            collective_id=0, has_side_effects=True, vmem_limit_bytes=VMEM_LIMIT
        ),
        cost_estimate=pl.CostEstimate(flops=flops, bytes_accessed=8 * bands * reach, transcendentals=0),
    )(orbitals, projectors, coupling, species, offsets)


def settle_kernel(src_ref, dst_ref, buf, in_sem, out_sem):
    pieces = in_sem.shape[0]
    rows = src_ref.shape[0] // pieces
    pulls, pushes = [], []
    for i in range(pieces):
        part = pl.ds(i * rows, rows)
        pulls.append(pltpu.make_async_copy(src_ref.at[part], buf.at[part], in_sem.at[i]))
        pushes.append(pltpu.make_async_copy(buf.at[part], dst_ref.at[part], out_sem.at[i]))
    for copy in pulls:
        copy.start()
    for pull, push in zip(pulls, pushes):
        pull.wait()
        push.start()
    for copy in pushes:
        copy.wait()


def settle(result, pieces):
    hbm = pl.BlockSpec(memory_space=pl.ANY)
    dma = pltpu.SemaphoreType.DMA
    return pl.pallas_call(
        settle_kernel,
        out_shape=jax.ShapeDtypeStruct(result.shape, result.dtype),
        in_specs=[hbm],
        out_specs=hbm,
        scratch_shapes=[pltpu.VMEM(result.shape, result.dtype), dma((pieces,)), dma((pieces,))],
        compiler_params=pltpu.CompilerParams(vmem_limit_bytes=VMEM_LIMIT),
        cost_estimate=pl.CostEstimate(flops=0, bytes_accessed=4 * result.size, transcendentals=0),
    )(result)


def per_device_kernel(groups, members, orbitals, projectors, coupling, species, offsets):
    chunks = orbitals.shape[0] // (groups * TILE)
    result = fused(
        chunks, members, orbitals, projectors, jnp.transpose(coupling, (1, 0, 2)), species[None, :], offsets[None, :]
    )
    return settle(result, 2 * chunks)


def per_device_plain(orbitals, projectors, coupling, species, offsets):
    total_proj = projectors.shape[0]
    p_real, p_imag = projectors[:, 0, :], projectors[:, 1, :]
    rows = coupling_rows(coupling, species, offsets, total_proj)
    matrix = block_diagonal(rows, *block_maps(total_proj, coupling.shape[1]))
    spread = lax.all_to_all(orbitals, "band", split_axis=2, concat_axis=0, tiled=True)
    o_real, o_imag = spread[:, 0, :], spread[:, 1, :]
    partial_sum = jnp.stack(
        [dot_t(o_real, p_real) + dot_t(o_imag, p_imag), dot_t(o_imag, p_real) - dot_t(o_real, p_imag)], axis=1
    )
    becp = lax.psum_scatter(partial_sum, ("ga", "band"), scatter_dimension=0, tiled=True)
    coupled = jnp.einsum("bcp,pq->bcq", becp, matrix, precision=lax.Precision.HIGHEST).astype(BF16)
    dbecp = lax.all_gather(coupled, ("ga", "band"), axis=0, tiled=True)
    d_real, d_imag = dbecp[:, 0, :], dbecp[:, 1, :]
    result = jnp.stack(
        [dot(d_real, p_real) - dot(d_imag, p_imag), dot(d_real, p_imag) + dot(d_imag, p_real)], axis=1
    ).astype(BF16)
    return lax.all_to_all(result, "band", split_axis=0, concat_axis=2, tiled=True)


def solution(mesh):
    groups, members = mesh.shape["ga"], mesh.shape["band"]

    def body(orbitals, projectors, *rest):
        fits = orbitals.shape[0] % (groups * TILE) == 0 and projectors.shape[0] % (2 * TILE) == 0
        if groups == 2 and members == PLANE * LINE and fits:
            return per_device_kernel(groups, members, orbitals, projectors, *rest)
        return per_device_plain(orbitals, projectors, *rest)

    placed = (P("band", None, "ga"), P(None, None, ("ga", "band")), P(), P(), P())
    return jax.shard_map(body, mesh=mesh, in_specs=placed, out_specs=P("band", None, "ga"), check_vma=False)
```

```python
import functools

import jax
import jax.numpy as jnp
import numpy as np
from jax import lax
from jax.experimental import pallas as pl
from jax.experimental.pallas import tpu as pltpu
from jax.sharding import PartitionSpec as P

MESH = pl.DeviceIdType.MESH
PLANE = 4
LINE = 4
TILE = 8
LANES = 128
F32 = jnp.float32
BF16 = jnp.bfloat16
VMEM_LIMIT = 63 * 1024 * 1024
WINDOW = 64
DELAYS = (
    (12, 16, 20, 24, 28),
    (12, 16, 20, 24, 28),
    (12, 16, 20, 25, 28),
    (12, 17, 20, 24, 28),
)


def coupling_rows(coupling, species, offsets, total_proj):
    kinds, per_atom = coupling.shape[0], coupling.shape[1]
    column = jnp.arange(total_proj, dtype=jnp.int32)
    within = column % per_atom
    start = column - within
    kind = jnp.sum(
        jnp.where(offsets[:, None] == start[None, :], species[:, None], 0), axis=0
    )
    pick = (jnp.arange(kinds * per_atom, dtype=jnp.int32)[:, None] == (kind * per_atom + within)[None, :])
    table = jnp.transpose(coupling, (2, 0, 1)).reshape(per_atom, kinds * per_atom)
    return jnp.dot(table, pick.astype(F32), precision=lax.Precision.HIGHEST, preferred_element_type=F32)


def block_diagonal(rows, spread, start_col, start_row):
    full = lax.dot_general(
        spread, rows, (((1,), (0,)), ((), ())), precision=lax.Precision.HIGHEST, preferred_element_type=F32
    )
    return jnp.where(start_col == start_row, full, 0.0)


def block_maps(count, per_atom):
    index = np.arange(count)
    spread = (index[:, None] % per_atom == np.arange(per_atom)[None, :]).astype(np.float32)
    start = (index // per_atom).astype(np.int32)
    return spread, start[:, None], start[None, :]


def dot_t(a, b):
    return lax.dot_general(a, b, (((1,), (1,)), ((), ())), preferred_element_type=F32)


def dot(a, b):
    return lax.dot_general(a, b, (((1,), (0,)), ((), ())), preferred_element_type=F32)


def flip(bit, by):
    return bit + by - 2 * bit * by


def kernel(
    chunks, o_ref, p_ref, coupling_ref, species_ref, offsets_ref, out_ref,
    obuf, praw, table, atoms, lbuf, pbuf, coef, zbuf, psend, precv, total, zsend, zrecv, hsum, hsend, hrecv, dbuf, rbuf,
    f_send, f_recv, l_sem, t_send, t_recv, p_send, p_recv, z_send, z_recv, h_send, h_recv,
    e_send, e_recv, d_send, d_recv, r_send, r_recv,
):
    g = lax.axis_index("ga")
    me = lax.axis_index("band")
    proj, wide = p_ref.shape[0], p_ref.shape[2]
    height, width = zbuf.shape[2], zbuf.shape[3]
    members = height // TILE
    quarter = height // PLANE
    half = quarter // 2
    per_atom = coupling_ref.shape[0]
    n, z = me % PLANE, me // PLANE
    x, y, z0, z1 = n % 2, n // 2, z % 2, z // 2

    def place(bx, by, b0, b1):
        return (b1 * 2 + b0) * PLANE + by * 2 + bx

    def slot(bx, by, b0, b1):
        return (by * 2 + bx) * LINE + b0 * 2 + b1

    def at(mask):
        bits = (flip(x, mask % 2), flip(y, (mask // 2) % 2), flip(z0, (mask // 4) % 2), flip(z1, mask // 8))
        return place(*bits), slot(*bits)

    my_slot = slot(x, y, z0, z1)
    twin = {"ga": 1 - g}
    plane = [(flip(x, j % 2), flip(y, j // 2)) for j in range(1, PLANE)]
    plane_at = [{"band": place(bx, by, z0, z1)} for bx, by in plane]
    near = {"band": place(x, y, 1 - z0, z1)}
    far = {"band": place(x, y, z0, 1 - z1)}
    peers = [None] + [at(mask) for mask in range(1, members)]

    def remote(src, dst, send, recv, to):
        return pltpu.make_async_remote_copy(
            src_ref=src, dst_ref=dst, send_sem=send, recv_sem=recv, device_id=to, device_id_type=MESH
        )

    barrier = pltpu.get_barrier_semaphore()
    pl.semaphore_signal(barrier, inc=1, device_id=twin, device_id_type=MESH)
    for mask in range(1, members):
        for core in range(2):
            pl.semaphore_signal(
                barrier, inc=1, device_id={"ga": core, "band": peers[mask][0]}, device_id_type=MESH
            )

    def piece(index, rows):
        return pl.ds(pl.multiple_of(index * rows, rows), rows)

    def rows_of(i, core):
        return piece(i * 2 + core, TILE)

    def cols_of(index):
        return piece(index, wide)

    my_rows = piece(my_slot, TILE)
    my_cols = cols_of(g)

    local = [
        pltpu.make_async_copy(p_ref, praw.at[g], l_sem.at[0]),
        pltpu.make_async_copy(coupling_ref, table, l_sem.at[1]),
        pltpu.make_async_copy(species_ref, atoms.at[0], l_sem.at[2]),
        pltpu.make_async_copy(offsets_ref, atoms.at[1], l_sem.at[3]),
    ]
    for copy in local:
        copy.start()
    for i in range(chunks):
        pltpu.make_async_copy(
            o_ref.at[rows_of(i, g), :, cols_of(me)], obuf.at[i, my_rows, :, my_cols], f_recv.at[i]
        ).start()

    pl.semaphore_wait(barrier, 2 * members - 1)

    twin_p = remote(p_ref, praw.at[g], t_send, t_recv, twin)

    def f_copy(i, q, core, peer, to, block=None):
        rows = rows_of(i, core if block is None else block)
        return remote(
            o_ref.at[rows, :, cols_of(peer)], obuf.at[i, my_rows, :, my_cols],
            f_send.at[i, q, core], f_recv.at[i], to,
        )

    def batch(q):
        inside = [q + 1] if q + 1 < PLANE else []
        return inside + [step * PLANE + q for step in range(1, members // PLANE)]

    def f_part(i, q, core):
        for mask in batch(q):
            peer, _ = peers[mask]
            f_copy(i, q, core, peer, {"ga": core, "band": peer}).start()

    def f_twin(i):
        f_copy(i, PLANE, 0, me, twin, 1 - g).start()

    def whole(ref, send, recv):
        return remote(ref, ref, send, recv, twin)

    def prepare():
        for copy in local:
            copy.wait()
        count = atoms.shape[2]
        turn = lax.broadcasted_iota(jnp.int32, (count, count), 0) == lax.broadcasted_iota(jnp.int32, (count, count), 1)

        def upright(row):
            return jnp.sum(jnp.where(turn, row.astype(F32), 0.0), axis=1, keepdims=True)

        column = lax.broadcasted_iota(jnp.int32, (count, width), 1).astype(F32)
        begin = upright(atoms[1])
        inside = (column >= begin) & (column < begin + per_atom)
        kind = jnp.sum(jnp.where(inside, upright(atoms[0]), 0.0), axis=0, keepdims=True)
        start = jnp.sum(jnp.where(inside, begin, 0.0), axis=0, keepdims=True)
        kind = (kind + 0.5).astype(jnp.int32)
        within = lax.broadcasted_iota(jnp.int32, (1, width), 1) - (start + 0.5).astype(jnp.int32)
        index = lax.broadcasted_iota(jnp.int32, (per_atom, width), 0)
        rows = jnp.zeros((per_atom, width), F32)
        for k in range(coupling_ref.shape[1]):
            pick = jnp.where((kind == k) & (within == index), 1.0, 0.0).astype(F32)
            rows = rows + lax.dot_general(
                table[:, k, :], pick, (((0,), (0,)), ((), ())),
                precision=lax.Precision.HIGHEST, preferred_element_type=F32,
            )
        for s in range(1 - per_atom, per_atom):
            coef[pl.ds(s + per_atom - 1, 1), :] = jnp.sum(
                jnp.where(index == within - s, rows, 0.0), axis=0, keepdims=True
            )
        twin_p.wait_recv()
        for c in range(2):
            for core in range(2):
                cols = pl.ds(core * wide, wide)
                if width > proj:
                    pbuf[c, pl.ds(proj, width - proj), cols] = jnp.zeros((width - proj, wide), BF16)

        def unpack(r, carry):
            rows = piece(r, 2 * TILE)
            for core in range(2):
                pbuf[:, rows, pl.ds(core * wide, wide)] = jnp.swapaxes(praw[core, rows], 0, 1)
            return carry

        lax.fori_loop(0, proj // (2 * TILE), unpack, 0)

    def blocks(count):
        step = 2 * LANES
        return [(low, min(step, count - low)) for low in range(0, count, step)]

    pcopy, zcopy, hcopy, ecopy, dcopy = {}, {}, {}, {}, {}

    def project(i):
        whole(obuf.at[i], f_send.at[i, 0, 0], f_recv.at[i]).wait_recv()
        for r in range(0, height, 2 * TILE):
            lbuf[:, pl.ds(r, 2 * TILE), :] = jnp.swapaxes(obuf[i, pl.ds(r, 2 * TILE)], 0, 1)
        left = lbuf[...].reshape(2 * height, 2 * wide)
        for low, size in blocks(width):
            a = dot_t(left, pbuf[0, pl.ds(low, size), :])
            b = dot_t(left, pbuf[1, pl.ds(low, size), :])
            zbuf[i, 0, :, pl.ds(low, size)] = a[:height] + b[height:]
            zbuf[i, 1, :, pl.ds(low, size)] = a[height:] - b[:height]
        for j in range(PLANE - 1):
            bx, by = plane[j]
            psend[i, j] = zbuf[i, :, piece(by * 2 + bx, quarter), :].astype(BF16)
            pcopy[i, j] = remote(psend.at[i, j], precv.at[i, j], p_send.at[i, j], p_recv.at[i, j], plane_at[j])
            pcopy[i, j].start()

    def reduce_plane(i):
        value = zbuf[i, :, piece(n, quarter), :]
        for j in range(PLANE - 1):
            pcopy[i, j].wait_recv()
            value = value + precv[i, j].astype(F32)
        total[i] = value
        zsend[i] = total[i, :, piece(1 - z0, half), :].astype(BF16)
        zcopy[i] = remote(zsend.at[i], zrecv.at[i], z_send.at[i], z_recv.at[i], near)
        zcopy[i].start()

    def reduce_near(i):
        zcopy[i].wait_recv()
        value = total[i, :, piece(z0, half), :] + zrecv[i].astype(F32)
        hsum[i] = value
        hsend[i] = value.astype(BF16)
        hcopy[i] = remote(hsend.at[i], hrecv.at[i], h_send.at[i], h_recv.at[i], far)
        hcopy[i].start()

    def couple(i):
        hcopy[i].wait_recv()
        value = (hsum[i] + hrecv[i].astype(F32)).reshape(2 * half, width)
        result = jnp.zeros_like(value)
        for s in range(1 - per_atom, per_atom):
            moved = value if s == 0 else pltpu.roll(value, s % width, 1)
            result = result + moved * coef[pl.ds(s + per_atom - 1, 1), :]
        mine = piece(n * 2 + z0, half)
        dbuf[i, :, mine, :] = result.astype(BF16).reshape(2, half, width)
        own = dbuf.at[i, :, mine, :]
        ecopy[i] = remote(own, own, e_send.at[i], e_recv.at[i], near)
        ecopy[i].start()
        for j in range(PLANE - 1):
            dcopy[i, 0, j] = remote(own, own, d_send.at[i, 0, j], d_recv.at[i, 0, j], plane_at[j])
            dcopy[i, 0, j].start()

    def hand_on(i):
        ecopy[i].wait_recv()
        got = dbuf.at[i, :, piece(n * 2 + 1 - z0, half), :]
        for j in range(PLANE - 1):
            dcopy[i, 1, j] = remote(got, got, d_send.at[i, 1, j], d_recv.at[i, 1, j], plane_at[j])
            dcopy[i, 1, j].start()

    def r_copy(i, q, core, there, to, block=None):
        return remote(
            rbuf.at[i, piece(there, TILE), :, cols_of(core if block is None else block)],
            out_ref.at[rows_of(i, g), :, cols_of(me)], r_send.at[i, q, core], r_recv.at[i], to,
        )

    def r_part(i, q, core):
        for mask in batch(q):
            peer, there = peers[mask]
            r_copy(i, q, core, there, {"ga": core, "band": peer}).start()

    def sent(k):
        phase, i, q, core = batches[k]
        ref = (obuf, rbuf)[phase].at[i, pl.ds(0, len(batch(q)) * TILE // 2)]
        send = (f_send, r_send)[phase].at[i, q, core]
        whole(ref, send, (f_recv, r_recv)[phase].at[i]).wait_send()

    def apply(i, core):
        if core == 0:
            for v in range(2):
                for j in range(PLANE - 1):
                    dcopy[i, v, j].wait_recv()
        left = dbuf[i].reshape(2 * height, width)
        for low, size in blocks(wide):
            cols = pl.ds(core * wide + low, size)
            a = dot(left, pbuf[0, :, cols])
            b = dot(left, pbuf[1, :, cols])
            both = jnp.stack([a[:height] - b[height:], b[:height] + a[height:]]).astype(BF16)
            for r in range(0, height, 2 * TILE):
                rbuf[i, pl.ds(r, 2 * TILE), :, cols] = jnp.swapaxes(both[:, r : r + 2 * TILE], 0, 1)
        if core == 1:
            r_copy(i, PLANE, 0, my_slot, twin, 1 - g).start()
            pltpu.make_async_copy(
                rbuf.at[i, my_rows, :, cols_of(g)], out_ref.at[rows_of(i, g), :, cols_of(me)], r_recv.at[i]
            ).start()

    batches = [
        (phase, i, q, core)
        for phase in range(2) for i in range(chunks) for core in range(2) for q in range(PLANE)
    ]
    each = 2 * PLANE
    stages = (project, reduce_plane, reduce_near, couple, hand_on)
    plan = {}
    for i in range(chunks):
        for stage, delay in zip(stages, DELAYS[min(i, len(DELAYS) - 1)]):
            plan.setdefault(min(i * each + delay, len(batches) // 2 + i * each), []).append((stage, i))

    twin_p.start()
    for k, (phase, i, q, core) in enumerate(batches):
        for stage, index in sorted(plan.get(k, []), key=lambda item: item[1]):
            stage(index)
        if k == each // 2:
            prepare()
        if k >= WINDOW:
            sent(k - WINDOW)
        if phase:
            if q == 0:
                apply(i, core)
            r_part(i, q, core)
        else:
            if core + q == 0:
                f_twin(i)
            f_part(i, q, core)

    for k in range(max(len(batches) - WINDOW, 0), len(batches)):
        sent(k)
    twin_p.wait_send()
    for copies in (pcopy, zcopy, hcopy, ecopy, dcopy):
        for copy in copies.values():
            copy.wait_send()
    single = pl.ds(0, TILE // 2)
    for i in range(chunks):
        whole(obuf.at[i, single], f_send.at[i, PLANE, 0], f_recv.at[i]).wait_send()
        whole(rbuf.at[i, single], r_send.at[i, PLANE, 0], r_recv.at[i]).wait_send()
        whole(out_ref.at[pl.ds(i * 2 * TILE, 2 * TILE)], r_send.at[i, PLANE, 0], r_recv.at[i]).wait_recv()


def fused(chunks, members, orbitals, projectors, coupling, species, offsets):
    bands, _, reach = orbitals.shape
    proj, _, wide = projectors.shape
    width = -(-proj // LANES) * LANES
    height = members * TILE
    quarter = height // PLANE
    half = quarter // 2
    per_atom = coupling.shape[0]
    taps = -(-(2 * per_atom - 1) // TILE) * TILE + TILE
    dma = pltpu.SemaphoreType.DMA
    hbm = pl.BlockSpec(memory_space=pl.ANY)
    flops = 64 * chunks * height * width * wide
    vm = pltpu.VMEM
    steps = dma((chunks,))
    return pl.pallas_call(
        functools.partial(kernel, chunks),
        out_shape=jax.ShapeDtypeStruct(orbitals.shape, BF16),
        in_specs=[hbm] * 5,
        out_specs=hbm,
        scratch_shapes=[
            vm((chunks, height, 2, 2 * wide), BF16),
            vm((2, proj, 2, wide), BF16),
            vm(coupling.shape, F32),
            vm((2,) + species.shape, jnp.int32),
            vm((2, height, 2 * wide), BF16),
            vm((2, width, 2 * wide), BF16),
            vm((taps, width), F32),
            vm((chunks, 2, height, width), F32),
            vm((chunks, PLANE - 1, 2, quarter, width), BF16),
            vm((chunks, PLANE - 1, 2, quarter, width), BF16),
            vm((chunks, 2, quarter, width), F32),
            vm((chunks, 2, half, width), BF16),
            vm((chunks, 2, half, width), BF16),
            vm((chunks, 2, half, width), F32),
            vm((chunks, 2, half, width), BF16),
            vm((chunks, 2, half, width), BF16),
            vm((chunks, 2, height, width), BF16),
            vm((chunks, height, 2, 2 * wide), BF16),
            dma((chunks, PLANE + 1, 2)), steps, dma((4,)), dma, dma,
            dma((chunks, PLANE - 1)), dma((chunks, PLANE - 1)),
            steps, steps, steps, steps, steps, steps,
            dma((chunks, 2, PLANE - 1)), dma((chunks, 2, PLANE - 1)),
            dma((chunks, PLANE + 1, 2)), steps,
        ],
        compiler_params=pltpu.CompilerParams(
            collective_id=0, has_side_effects=True, vmem_limit_bytes=VMEM_LIMIT
        ),
        cost_estimate=pl.CostEstimate(flops=flops, bytes_accessed=8 * bands * reach, transcendentals=0),
    )(orbitals, projectors, coupling, species, offsets)


def settle_kernel(src_ref, dst_ref, buf, in_sem, out_sem):
    pieces = in_sem.shape[0]
    rows = src_ref.shape[0] // pieces
    pulls, pushes = [], []
    for i in range(pieces):
        part = pl.ds(i * rows, rows)
        pulls.append(pltpu.make_async_copy(src_ref.at[part], buf.at[part], in_sem.at[i]))
        pushes.append(pltpu.make_async_copy(buf.at[part], dst_ref.at[part], out_sem.at[i]))
    for copy in pulls:
        copy.start()
    for pull, push in zip(pulls, pushes):
        pull.wait()
        push.start()
    for copy in pushes:
        copy.wait()


def settle(result, pieces):
    hbm = pl.BlockSpec(memory_space=pl.ANY)
    dma = pltpu.SemaphoreType.DMA
    return pl.pallas_call(
        settle_kernel,
        out_shape=jax.ShapeDtypeStruct(result.shape, result.dtype),
        in_specs=[hbm],
        out_specs=hbm,
        scratch_shapes=[pltpu.VMEM(result.shape, result.dtype), dma((pieces,)), dma((pieces,))],
        compiler_params=pltpu.CompilerParams(vmem_limit_bytes=VMEM_LIMIT),
        cost_estimate=pl.CostEstimate(flops=0, bytes_accessed=4 * result.size, transcendentals=0),
    )(result)


def per_device_kernel(groups, members, orbitals, projectors, coupling, species, offsets):
    chunks = orbitals.shape[0] // (groups * TILE)
    result = fused(
        chunks, members, orbitals, projectors, jnp.transpose(coupling, (1, 0, 2)), species[None, :], offsets[None, :]
    )
    return settle(result, 2 * chunks)


def per_device_plain(orbitals, projectors, coupling, species, offsets):
    total_proj = projectors.shape[0]
    p_real, p_imag = projectors[:, 0, :], projectors[:, 1, :]
    rows = coupling_rows(coupling, species, offsets, total_proj)
    matrix = block_diagonal(rows, *block_maps(total_proj, coupling.shape[1]))
    spread = lax.all_to_all(orbitals, "band", split_axis=2, concat_axis=0, tiled=True)
    o_real, o_imag = spread[:, 0, :], spread[:, 1, :]
    partial_sum = jnp.stack(
        [dot_t(o_real, p_real) + dot_t(o_imag, p_imag), dot_t(o_imag, p_real) - dot_t(o_real, p_imag)], axis=1
    )
    becp = lax.psum_scatter(partial_sum, ("ga", "band"), scatter_dimension=0, tiled=True)
    coupled = jnp.einsum("bcp,pq->bcq", becp, matrix, precision=lax.Precision.HIGHEST).astype(BF16)
    dbecp = lax.all_gather(coupled, ("ga", "band"), axis=0, tiled=True)
    d_real, d_imag = dbecp[:, 0, :], dbecp[:, 1, :]
    result = jnp.stack(
        [dot(d_real, p_real) - dot(d_imag, p_imag), dot(d_real, p_imag) + dot(d_imag, p_real)], axis=1
    ).astype(BF16)
    return lax.all_to_all(result, "band", split_axis=0, concat_axis=2, tiled=True)


def solution(mesh):
    groups, members = mesh.shape["ga"], mesh.shape["band"]

    def body(orbitals, projectors, *rest):
        fits = orbitals.shape[0] % (groups * TILE) == 0 and projectors.shape[0] % (2 * TILE) == 0
        if groups == 2 and members == PLANE * LINE and fits:
            return per_device_kernel(groups, members, orbitals, projectors, *rest)
        return per_device_plain(orbitals, projectors, *rest)

    placed = (P("band", None, "ga"), P(None, None, ("ga", "band")), P(), P(), P())
    return jax.shard_map(body, mesh=mesh, in_specs=placed, out_specs=P("band", None, "ga"), check_vma=False)
```
